32 devices in a mesh: seq: 8 (over z, y), grp: 4 (over x, core).
Axes of the slice: x: 2, y: 2, z: 4, core: 2. Of those that a mesh axis runs over, the one named last changes fastest.
Arguments:
- frames: bfloat16 [16384, 1024], P(('seq', 'grp')), may hold values from -6 to 6
- ln1_gain: float32 [1024], replicated, may hold values from 0.1 to 1.9
- w_in: bfloat16 [1024, 2, 1024], P('seq', None, 'grp'), may hold values from -0.1875 to 0.1875
- w_dw: bfloat16 [31, 1024], replicated, may hold values from -1 to 1
- ln2_gain: float32 [1024], replicated, may hold values from 0.1 to 1.9
- ln2_bias: float32 [1024], replicated, may hold values from -3 to 3
- w_out: bfloat16 [1024, 1024], P('grp', 'seq'), may hold values from -0.1875 to 0.1875
- block_utt: int32 [128], replicated, may hold values from 0 to 31, as said below
- block_off: int32 [128], replicated, may hold values from 0 to 6, as said below
- lengths: int32 [32], replicated, may hold values from 1 to 896, as said below
Outputs:
- result: bfloat16 [16384, 1024], P(('seq', 'grp'))
The draws below stay inside these ranges and needn't reach their ends.
Inputs may be any that keep to these rules, and one draw needn't show every extreme that they name: block_utt never falls along the blocks and names every utterance; each utterance is one run of 1 to 7 whole blocks, and some utterance has exactly 7. block_off counts the blocks of the run before a block, starting at 0. `lengths`: an utterance of n blocks has more than (n - 1) * 128 and at most n * 128 live frames.
All inputs are finite; a program needn't handle non-finite values.
Results may differ from the reference program's by a relative error of at most 0.0046.
Values may be sent and summed in bfloat16 or wider, within the bound.
A program may use at most 64 MiB of HBM per device.

```python
import jax
import jax.numpy as jnp
from jax import lax

D = 1024
KER = 31
BLK = 128
FRAMES = 16384
NBLK = 128
UTTS = 32
N_SEQ = 8


def layout_tables(key):
    base = jax.random.fold_in(key, 7)
    first_key, second_key = jax.random.split(base)
    pattern = jnp.array([-3, -2, -1, 0, 0, 1, 2, 3], jnp.int32)
    offsets = jnp.tile(pattern, UTTS // 8)
    order = jax.random.permutation(first_key, UTTS)
    counts = (4 + jnp.take(offsets, order)).astype(jnp.int32)
    ends = jnp.cumsum(counts).astype(jnp.int32)
    starts = (ends - counts).astype(jnp.int32)
    indices = jnp.arange(NBLK, dtype=jnp.int32)
    block_utt = jnp.sum((ends[None, :] <= indices[:, None]).astype(jnp.int32), axis=1).astype(jnp.int32)
    block_off = (indices - jnp.take(starts, block_utt)).astype(jnp.int32)
    tails = jax.random.randint(second_key, (UTTS,), 1, BLK + 1, dtype=jnp.int32)
    tails = jnp.where(counts == 7, BLK, tails).astype(jnp.int32)
    lengths = ((counts - 1) * BLK + tails).astype(jnp.int32)
    return (block_utt, block_off, lengths)


def draw_block_utt(key, part):
    return layout_tables(key)[0]


def draw_block_off(key, part):
    return layout_tables(key)[1]


def draw_lengths(key, part):
    return layout_tables(key)[2]


def shard_levels(rng, shape, shards, least, high):
    level = 1.0
    for dim, shards_of in shards:
        steps = jax.random.uniform(jax.random.fold_in(jax.random.fold_in(rng, 6), dim), (shards_of,), jnp.float32, least / len(shards), high / len(shards))
        level = level * jnp.repeat(jnp.exp(steps), shape[dim] // shards_of).reshape((-1,) + (1,) * (len(shape) - 1 - dim))
    return level


def noise(own_key, extent, scale, reach, cuts=(), held_as=jnp.bfloat16):
    loudness = shard_levels(own_key, extent, cuts, -0.22, 0.18) if cuts else 1.0
    values = jax.random.normal(own_key, extent, jnp.float32) * scale * loudness
    return jnp.minimum(jnp.maximum(values, -reach), reach).astype(held_as)


def setup_inputs(seed: int = 0) -> dict:
    key_of = jax.random.split(jax.random.key(seed), 11)
    return {
        "frames": noise(key_of[0], (FRAMES, D), 1.0, 6.0, ((0, 32),)),
        "ln1_gain": jnp.clip(1.0 + 0.18 * jax.random.normal(key_of[1], (D,), jnp.float32), 0.1, 1.9),
        "w_in": noise(key_of[2], (D, 2, D), D ** -0.5, 0.1875, ((0, 8), (2, 4))),
        "w_dw": noise(key_of[3], (KER, D), KER ** -0.5, 1.0),
        "ln2_gain": jnp.clip(1.0 + 0.18 * jax.random.normal(key_of[4], (D,), jnp.float32), 0.1, 1.9),
        "ln2_bias": noise(key_of[5], (D,), 0.5, 3.0, (), jnp.float32),
        "w_out": noise(key_of[6], (D, D), D ** -0.5, 0.1875, ((0, 4), (1, 8))),
        "block_utt": draw_block_utt(jax.random.fold_in(key_of[10], 71), 0),
        "block_off": draw_block_off(jax.random.fold_in(key_of[10], 71), 0),
        "lengths": draw_lengths(jax.random.fold_in(key_of[10], 71), 0),
    }


epsilon = 1e-05

def frame_keys(block_utt, block_off, lengths, first_row, row_count, margin):
    places = first_row - margin + jnp.arange(row_count + 2 * margin, dtype=jnp.int32)
    total_rows = block_utt.shape[0] * BLK
    inside = (places >= 0) & (places < total_rows)
    blocks = jnp.clip(places // BLK, 0, block_utt.shape[0] - 1)
    utterance = jnp.take(block_utt, blocks)
    position = jnp.take(block_off, blocks) * BLK + places % BLK
    living = inside & (position < jnp.take(lengths, utterance))
    return (jnp.where(living, utterance, -1), living[margin:margin + row_count])

def layer_norm(rows, gain):
    values = rows.astype(jnp.float32)
    average = lax.optimization_barrier(jnp.mean(values, axis=1, keepdims=True))
    centered = values - average
    spread = lax.optimization_barrier(jnp.mean(centered * centered, axis=1, keepdims=True))
    return (centered * lax.rsqrt(spread + epsilon) * gain).astype(jnp.bfloat16)

def gate_units(projected, living):
    half = projected.shape[1] // 2
    values = projected[:, :half] * jax.nn.sigmoid(projected[:, half:])
    return (values * living.astype(jnp.float32)[:, None]).astype(jnp.bfloat16)

def depthwise(widened, keys_wide, taps, row_count):
    margin = (taps.shape[0] - 1) // 2
    center = keys_wide[margin:margin + row_count]
    summed = jnp.zeros((row_count, widened.shape[1]), jnp.float32)
    for tap_index in range(taps.shape[0]):
        shifted = widened[tap_index:tap_index + row_count].astype(jnp.float32)
        same = (keys_wide[tap_index:tap_index + row_count] == center)[:, None]
        summed = summed + jnp.where(same, shifted, 0.0) * taps[tap_index].astype(jnp.float32)
    return summed

def finish(mixed, stat_sum, square_sum, width_total, gain, bias):
    average = stat_sum / width_total
    spread = square_sum / width_total - average * average
    normed = (mixed - average[:, None]) * lax.rsqrt(spread + epsilon)[:, None] * gain + bias
    return (normed * jax.nn.sigmoid(normed)).astype(jnp.bfloat16)

def reference(frames, ln1_gain, w_in, w_dw, ln2_gain, ln2_bias, w_out, block_utt, block_off, lengths):
    margin = (KER - 1) // 2
    keys_wide, living = frame_keys(block_utt, block_off, lengths, 0, FRAMES, margin)
    w_flat = w_in.reshape(D, 2 * D)

    def first_half(pair):
        rows, alive = pair
        normed = layer_norm(rows, ln1_gain)
        projected = jnp.dot(normed, w_flat, preferred_element_type=jnp.float32)
        return gate_units(projected, alive)
    gated = lax.map(first_half, (frames.reshape(N_SEQ, -1, D), living.reshape(N_SEQ, -1))).reshape(FRAMES, D)
    widened = jnp.pad(gated, ((margin, margin), (0, 0)))
    mixed = depthwise(widened, keys_wide, w_dw, FRAMES)

    def second_half(triple):
        rows, alive, mixed_rows = triple
        act = finish(mixed_rows, lax.optimization_barrier(jnp.sum(mixed_rows, axis=1)), lax.optimization_barrier(jnp.sum(mixed_rows * mixed_rows, axis=1)), float(D), ln2_gain, ln2_bias)
        output = jnp.dot(act, w_out, preferred_element_type=jnp.float32)
        return (rows.astype(jnp.float32) + output * alive.astype(jnp.float32)[:, None]).astype(jnp.bfloat16)
    result = lax.map(second_half, (frames.reshape(N_SEQ, -1, D), living.reshape(N_SEQ, -1), mixed.reshape(N_SEQ, -1, D)))
    return result.reshape(FRAMES, D)
```

```python
import functools

import jax
import jax.numpy as jnp
from jax import lax
from jax.experimental import pallas as pl
from jax.experimental.pallas import tpu as pltpu
from jax.sharding import PartitionSpec as P

D = 1024
KER = 31
BLK = 128


epsilon = 1e-05


def extended(block, sides, width):
    for axis, dim in sides:
        count = lax.axis_size(axis)
        forward = [(i, i + 1) for i in range(count - 1)]
        backward = [(target, source) for source, target in forward]
        low = lax.ppermute(
            lax.slice_in_dim(block, block.shape[dim] - width, None, axis=dim), axis, forward
        )
        high = lax.ppermute(lax.slice_in_dim(block, 0, width, axis=dim), axis, backward)
        block = jnp.concatenate([low, block, high], axis=dim)
    return block


def frame_keys(block_utt, block_off, lengths, first_row, row_count, margin):
    places = first_row - margin + jnp.arange(row_count + 2 * margin, dtype=jnp.int32)
    total_rows = block_utt.shape[0] * BLK
    inside = (places >= 0) & (places < total_rows)
    blocks = jnp.clip(places // BLK, 0, block_utt.shape[0] - 1)
    utterance = jnp.take(block_utt, blocks)
    position = jnp.take(block_off, blocks) * BLK + places % BLK
    living = inside & (position < jnp.take(lengths, utterance))
    return (jnp.where(living, utterance, -1), living[margin : margin + row_count])


def layer_norm(rows, gain):
    values = rows.astype(jnp.float32)
    average = jnp.mean(values, axis=1, keepdims=True)
    centered = values - average
    spread = jnp.mean(centered * centered, axis=1, keepdims=True)
    return (centered * lax.rsqrt(spread + epsilon) * gain).astype(jnp.bfloat16)


def gate_units(projected, living):
    half = projected.shape[1] // 2
    values = projected[:, :half] * jax.nn.sigmoid(projected[:, half:])
    return (values * living.astype(jnp.float32)[:, None]).astype(jnp.bfloat16)


def depthwise(widened, keys_wide, taps, row_count):
    margin = (taps.shape[0] - 1) // 2
    center = keys_wide[margin : margin + row_count]
    summed = jnp.zeros((row_count, widened.shape[1]), jnp.float32)
    for tap_index in range(taps.shape[0]):
        shifted = widened[tap_index : tap_index + row_count].astype(jnp.float32)
        same = (keys_wide[tap_index : tap_index + row_count] == center)[:, None]
        summed = summed + jnp.where(same, shifted, 0.0) * taps[tap_index].astype(jnp.float32)
    return summed


def finish(mixed, stat_sum, square_sum, width_total, gain, bias):
    average = stat_sum / width_total
    spread = square_sum / width_total - average * average
    normed = (mixed - average[:, None]) * lax.rsqrt(spread + epsilon)[:, None] * gain + bias
    return (normed * jax.nn.sigmoid(normed)).astype(jnp.bfloat16)


def project_rows(normed, row_count, column_count):

    def add_rows(total, weight_piece, start_row):
        piece_rows = weight_piece.shape[0]
        return jnp.dot(
            normed, weight_piece.reshape(piece_rows, -1), preferred_element_type=jnp.float32
        )

    return (add_rows, jnp.zeros((row_count, column_count), jnp.float32))


def per_device(
    frames, ln1_gain, w_in, w_dw, ln2_gain, ln2_bias, w_out, block_utt, block_off, lengths
):
    row_count = frames.shape[0]
    margin = (KER - 1) // 2
    own_first = lax.axis_index(("seq", "grp")) * row_count
    keys_wide, living = frame_keys(block_utt, block_off, lengths, own_first, row_count, margin)
    normed = layer_norm(frames, ln1_gain)
    w_in_rows, w_out_rows = (
        lax.all_gather(w_in, "grp", axis=2, tiled=True),
        lax.all_gather(w_out, "grp", axis=0, tiled=True),
    )
    add_rows, empty = project_rows(normed, row_count, 2 * D)
    projected = add_rows(empty, lax.all_gather(w_in_rows, "seq", axis=0, tiled=True), jnp.int32(0))
    gated = gate_units(projected, living)
    widened = extended(gated, ((("seq", "grp"), 0),), margin)
    mixed = depthwise(widened, keys_wide, w_dw, row_count)
    act = finish(
        mixed, jnp.sum(mixed, axis=1), jnp.sum(mixed * mixed, axis=1), float(D), ln2_gain, ln2_bias
    )
    output = jnp.dot(
        act,
        lax.all_gather(w_out_rows, "seq", axis=1, tiled=True),
        preferred_element_type=jnp.float32,
    )
    alive = living.astype(jnp.float32)[:, None]
    return (frames.astype(jnp.float32) + output * alive).astype(jnp.bfloat16)


MESH = pl.DeviceIdType.MESH
HALO = 16
LANES = 128
PLANES = 4
O, X, Y, CX, CY, CZ, PP = (PLANES * i for i in range(7))
KINDS = 7 * PLANES + 8
COMPUTE = True

ORDER = (
    "Q0", "R0", "Q1", "N0", "XY00", "B00", "R1", "B01", "N1", "C00",
    "XY10", "Q2", "XY01", "B02", "B10", "B11", "G00", "halo", "K000", "C01",
    "D0", "C10", "L0", "XY11", "P00", "B12", "R2", "G10", "K010", "XY20",
    "L1", "C11", "D1", "G01", "K001", "B20", "L2", "P10", "B21", "K100",
    "C20", "G11", "P01", "XY21", "B22", "K011", "C21", "D2", "K110", "P11",
    "S0", "S1", "S2", "K101", "S3", "K111", "L3", "fin",
)


def fused_kernel(
    frames_hbm,
    wi_own,
    wo_own,
    gain1,
    taps,
    gain2,
    bias2,
    utts,
    offs,
    lens,
    out,
    WI,
    WO,
    FR,
    HB,
    NM,
    NH,
    GB0,
    GB1,
    MX,
    TP,
    ACT,
    S1,
    S2,
    limits,
    edge_limits,
    edge_joined,
    ssem,
    rsem,
    hs,
    hr,
    lsem,
):
    rows, width = FR.shape
    krows = wi_own.shape[0]
    nblk = rows // BLK
    chunks = width // LANES
    seq = lax.axis_index("seq")
    grp = lax.axis_index("grp")
    nseq = lax.axis_size("seq")
    ngrp = lax.axis_size("grp")
    z, y = seq // 2, seq % 2
    x, c = grp // 2, grp % 2
    index = seq * ngrp + grp
    total = nseq * ngrp
    hi, lo = z // 2, z % 2
    end = 1 - hi - lo + 2 * hi * lo
    near = 2 * hi + 1 - lo
    item_at = (z, 3 - z, near, 3 - near)
    source_at = (
        end * near + (1 - end) * (3 - z),
        end * (3 - z) + (1 - end) * near,
        3 - near,
    )

    px = (seq, (1 - x) * 2 + c)
    py = (z * 2 + 1 - y, grp)
    pp = (seq, x * 2 + 1 - c)
    has_next = index < total - 1
    has_before = index > 0
    after = jnp.minimum(index + 1, total - 1)
    before = jnp.maximum(index - 1, 0)
    pn = (after // ngrp, after % ngrp)
    pb = (before // ngrp, before % ngrp)

    def plane(t):
        return (t * 2 + y, grp)

    load = pltpu.make_async_copy(frames_hbm, FR, lsem.at[0])
    load.start()

    barrier = pltpu.get_barrier_semaphore()
    peers = [px, py, pp] + [plane((z + k) % PLANES) for k in range(1, PLANES)]
    for peer in peers:
        pl.semaphore_signal(barrier, inc=1, device_id=peer, device_id_type=MESH)

    @pl.when(has_next)
    def _():
        pl.semaphore_signal(barrier, inc=1, device_id=pn, device_id_type=MESH)

    @pl.when(has_before)
    def _():
        pl.semaphore_signal(barrier, inc=1, device_id=pb, device_id_type=MESH)

    @pl.when(jnp.logical_not(has_before))
    def _():
        HB[0] = jnp.zeros((HALO, width), jnp.bfloat16)

    @pl.when(jnp.logical_not(has_next))
    def _():
        HB[1] = jnp.zeros((HALO, width), jnp.bfloat16)

    own_rows = pl.ds(pl.multiple_of(seq * krows, krows), krows)
    for h in range(2):
        WI[h, c, x, own_rows, :] = wi_own[:, h * 2 * LANES : (h + 1) * 2 * LANES]
    WO[c, z, y, x] = wo_own[...]
    pl.semaphore_wait(
        barrier, len(peers) + has_next.astype(jnp.int32) + has_before.astype(jnp.int32)
    )

    def slot(w, sx, sy, sz, half=None):
        if w < 2:
            count = krows if half is None else krows // 2
            first = (sz * 2 + sy) * krows + (0 if half is None else half * count)
            return WI.at[w, c, sx, pl.ds(pl.multiple_of(first, count), count), :]
        if half is None:
            return WO.at[c, sz, sy, sx]
        count = WO.shape[4] // 2
        return WO.at[c, sz, sy, sx, pl.ds(half * count, count), :]

    sent = []
    middle_sent = []

    def copy(w, ref, sem, dev):
        return pltpu.make_async_remote_copy(
            src_ref=ref,
            dst_ref=ref,
            send_sem=ssem.at[w, len(sent) % KINDS],
            recv_sem=rsem.at[w, sem],
            device_id=dev,
            device_id_type=MESH,
        )

    count_of = [0, 0, 0]

    def send(w, ref, sem, dev):
        made = pltpu.make_async_remote_copy(
            src_ref=ref,
            dst_ref=ref,
            send_sem=ssem.at[w, count_of[w]],
            recv_sem=rsem.at[w, sem],
            device_id=dev,
            device_id_type=MESH,
        )
        made.start()
        count_of[w] += 1
        sent.append(made)

    def receive(w, ref, sem):
        copy(w, ref, sem, px).wait_recv()

    def middle_send(w, ref, sem, dev):
        made = pltpu.make_async_remote_copy(
            src_ref=ref,
            dst_ref=ref,
            send_sem=ssem.at[w, count_of[w]],
            recv_sem=rsem.at[w, sem],
            device_id=dev,
            device_id_type=MESH,
        )
        count_of[w] += 1
        middle_sent.append(made)

        @pl.when(end == 0)
        def _():
            made.start()

    def own_square(w):
        ref = slot(w, x, y, z)
        send(w, ref, X + z, px)
        send(w, ref, Y + z, py)

    def own_line(w):
        ref = slot(w, x, y, z)
        send(w, ref, O + z, plane(3 - z))
        send(w, ref, O + z, plane(near))

    def line(w, p):
        s = source_at[p]
        ref = slot(w, x, y, s)
        receive(w, ref, O + s)
        if p == 0:
            middle_send(w, slot(w, x, y, 3 - z), O + 3 - z, plane(near))
        if p == 1:
            middle_send(w, slot(w, x, y, near), O + near, plane(3 - z))
        send(w, ref, X + s, px)
        send(w, ref, Y + s, py)

    def corner_relay(w):
        ref = slot(w, 1 - x, 1 - y, near)
        receive(w, ref, CZ + near)
        middle_send(w, ref, CZ + near, plane(3 - z))

    def corner_sends(w, i):
        s = item_at[i]
        receive(w, slot(w, x, 1 - y, s), Y + s)
        send(w, slot(w, x, 1 - y, s, 0), CX + s, px)
        receive(w, slot(w, 1 - x, y, s), X + s)
        send(w, slot(w, 1 - x, y, s, 1), CY + s, py)

    def corner(w, i):
        s = item_at[i]
        receive(w, slot(w, 1 - x, 1 - y, s, 0), CX + s)
        receive(w, slot(w, 1 - x, 1 - y, s, 1), CY + s)
        if i == 0:
            send(w, slot(w, 1 - x, 1 - y, s), CZ + s, plane(near))
        else:
            middle_send(w, slot(w, 1 - x, 1 - y, s), CZ + s, plane(near))

    def group(w, rel):
        if rel == 0:
            for s in item_at[2:]:
                receive(w, slot(w, x, 1 - y, s), Y + s)
            send(w, WI.at[w, c, x], PP, pp)
        else:
            for s in item_at[2:]:
                receive(w, slot(w, 1 - x, y, s), X + s)
            receive(w, slot(w, 1 - x, 1 - y, 3 - near), CZ + 3 - near)
            send(w, WI.at[w, c, 1 - x], PP + 1, pp)

    def group_partner(w, rel):
        receive(w, WI.at[w, 1 - c, x if rel == 0 else 1 - x], PP + rel)

    def column(i):
        s = item_at[i]
        if i >= 2:
            receive(2, slot(2, x, 1 - y, s), Y + s)
            receive(2, slot(2, 1 - x, y, s), X + s)
        if i == 3:
            receive(2, slot(2, 1 - x, 1 - y, s), CZ + s)
        send(2, WO.at[c, s], PP + s, pp)

    def halo_copy(src, dst, sem, dev):
        return pltpu.make_async_remote_copy(
            src_ref=src,
            dst_ref=dst,
            send_sem=hs.at[sem],
            recv_sem=hr.at[sem],
            device_id=dev,
            device_id_type=MESH,
        )

    to_next = halo_copy(FR.at[pl.ds(rows - HALO, HALO), :], HB.at[0], 0, pn)
    to_before = halo_copy(FR.at[pl.ds(0, HALO), :], HB.at[1], 1, pb)

    def halo_start():
        @pl.when(has_next)
        def _():
            to_next.start()

        @pl.when(has_before)
        def _():
            to_before.start()

    def norm_rows(block):
        values = block.astype(jnp.float32)
        average = jnp.mean(values, axis=1, keepdims=True)
        centered = values - average
        spread_ = jnp.mean(centered * centered, axis=1, keepdims=True)
        return (centered * lax.rsqrt(spread_ + epsilon) * gain1[...]).astype(jnp.bfloat16)

    tall_rows = BLK
    pack = 2 * 8

    def tile(ref, first, ch):
        return ref[pl.ds(first, pack), ch * LANES : (ch + 1) * LANES].astype(jnp.float32)

    def row_sum(parts):
        total_ = parts[0]
        for part in parts[1:]:
            total_ = total_ + part
        return jnp.sum(total_, axis=1, keepdims=True)

    def norm(step):
        def bands(i):
            return [
                pl.multiple_of(i * tall_rows + r * pack, pack) for r in range(tall_rows // pack)
            ]

        def average_step(i, carry):
            for first in bands(i):
                average = row_sum([tile(FR, first, ch) for ch in range(chunks)]) / float(width)
                S1[pl.ds(first, pack), :] = jnp.broadcast_to(average, (pack, LANES))
            return carry

        def spread_step(i, carry):
            for first in bands(i):
                average = S1[pl.ds(first, pack), :]
                parts = [tile(FR, first, ch) - average for ch in range(chunks)]
                spread = row_sum([p * p for p in parts]) / float(width)
                scale = lax.rsqrt(spread + epsilon)
                S2[pl.ds(first, pack), :] = jnp.broadcast_to(scale, (pack, LANES))
            return carry

        def scale_step(i, carry):
            for first in bands(i):
                average = S1[pl.ds(first, pack), :]
                scale = S2[pl.ds(first, pack), :]
                for ch in range(chunks):
                    cols = slice(ch * LANES, (ch + 1) * LANES)
                    NM[pl.ds(first, pack), cols] = (
                        (tile(FR, first, ch) - average) * scale * gain1[:, cols]
                    ).astype(jnp.bfloat16)
            return carry

        count = rows // tall_rows // 2
        for stage in (average_step, spread_step, scale_step):
            lax.fori_loop(count * step, count * (step + 1), stage, 0)

    def halo():
        @pl.when(has_before)
        def _():
            to_next.wait_recv()

        @pl.when(has_next)
        def _():
            to_before.wait_recv()

        NH[0:HALO, :] = norm_rows(HB[0])
        NH[HALO:, :] = norm_rows(HB[1])

    first_block = index * nblk
    last_block = total * nblk - 1

    def block_info(b):
        u = utts[b]
        return u, lens[u] - offs[b] * BLK

    info = [
        block_info(jnp.clip(first_block + i, 0, last_block)) for i in range(-1, nblk + 1)
    ]
    joined = []
    for i in range(nblk + 1):
        same = info[i][0] == info[i + 1][0]
        if i == 0:
            same = same & (first_block > 0)
        if i == nblk:
            same = same & (first_block + nblk <= last_block)
        joined.append(same.astype(jnp.float32))
    alive_rows = [info[i + 1][1] for i in range(nblk)]
    for i in range(nblk):
        limits[i] = alive_rows[i]
    edge_limits[0] = info[0][1] - (BLK - HALO)
    edge_limits[1] = info[nblk + 1][1]
    edge_joined[0] = joined[0]
    edge_joined[1] = joined[nblk]

    def tall(count, start):
        return start + lax.broadcasted_iota(jnp.int32, (count, LANES), 0)

    stride = BLK + 2 * HALO

    def chunk_of(h, rel_c, rel_x):
        cc = c if rel_c == 0 else 1 - c
        xx = x if rel_x == 0 else 1 - x
        return cc, xx, (xx * 2 + cc) * 2 + h

    started = []
    pending = []
    deep = 4
    part_rows = 16 * deep
    parts = BLK // part_rows

    def convolve_step(j, ch, buf, fresh, tap):
        i, q = j // (2 * parts), j % (2 * parts)
        base = pl.multiple_of(i * stride + q * (8 * deep), 8)
        sums = [None] * deep
        for o in range(8 * (deep - 1) + KER):
            value = buf[pl.ds(base + (1 + o), 8), :]
            for t in range(deep):
                k = o - 8 * t
                if 0 <= k < KER:
                    term = value * tap[k]
                    sums[t] = term if sums[t] is None else sums[t] + term
        first = pl.multiple_of(j * (8 * deep), 8 * deep)
        for t in range(deep):
            band = pl.ds(pl.multiple_of(first + 8 * t, 8), 8)
            MX[ch, band, :] = sums[t]
            if fresh:
                S1[band, :] = sums[t]
                S2[band, :] = sums[t] * sums[t]
            else:
                S1[band, :] += sums[t]
                S2[band, :] += sums[t] * sums[t]

    def work(project_id):
        earlier = pending.pop() if pending else None
        if earlier is None and project_id is None:
            return
        if earlier is not None:
            old_ch, old_buf, fresh = earlier
            tap = [jnp.broadcast_to(TP[old_ch, k : k + 1, :], (8, LANES)) for k in range(KER)]
        if project_id is not None:
            h = project_id[0]
            cc, xx, ch = chunk_of(*project_id)
            buf = (GB0, GB1)[len(started) % 2]
            pending.append((ch, buf, not started))
            started.append(ch)

        def gated(p):
            half = 0.5 * p[:, :LANES]
            return half + half * jnp.tanh(0.5 * p[:, LANES:])

        def rounded(units):
            return units.astype(jnp.bfloat16).astype(jnp.float32)

        def at_once(between):
            lhs = jnp.concatenate([NM[...], NH[...]], axis=0)
            p = jnp.dot(lhs, WI[h, cc, xx], preferred_element_type=jnp.float32)
            between()
            units = gated(p)
            for i in range(nblk):
                main = jnp.where(tall(BLK, 0) < alive_rows[i], units[i * BLK : (i + 1) * BLK], 0.0)
                buf[i * stride + HALO : i * stride + HALO + BLK, :] = rounded(main)
            for q in range(2):
                strip = units[rows + q * HALO : rows + (q + 1) * HALO]
                strip = rounded(jnp.where(tall(HALO, 0) < edge_limits[q], strip, 0.0))
                place = q * (nblk * stride - HALO)
                buf[place : place + HALO, :] = strip * edge_joined[q]

        def convolve(steps):
            for j in steps:
                convolve_step(j, old_ch, old_buf, fresh, tap)

        count = 2 * nblk * parts
        if earlier is None:
            at_once(lambda: None)
        elif project_id is None:

            def step(j, carry):
                convolve((2 * j, 2 * j + 1))
                return carry

            lax.fori_loop(0, count // 2, step, 0)
        else:
            at_once(lambda: convolve(range(count)))
        if project_id is not None:
            for i in range(1, nblk):
                base = i * stride
                buf[base : base + HALO, :] = (
                    buf[base - 2 * HALO : base - HALO, :] * joined[i]
                )
                buf[base - HALO : base, :] = (
                    buf[base + HALO : base + 2 * HALO, :] * joined[i]
                )

    wide = 2 * LANES

    def finish_all():
        half = WO.shape[3] * WO.shape[4]
        for s in item_at:
            receive(2, WO.at[1 - c, s], PP + s)
        if not COMPUTE:
            return
        for b in range(nblk):
            stats = []
            for r in range(tall_rows // pack):
                band = slice(b * BLK + r * pack, b * BLK + (r + 1) * pack)
                average = jnp.sum(S1[band, :], axis=1, keepdims=True) / float(width)
                square = jnp.sum(S2[band, :], axis=1, keepdims=True) / float(width)
                scale = lax.rsqrt(square - average * average + epsilon)
                stats.append((band, average, scale))
            for ch in range(chunks):
                cols = slice(ch * LANES, (ch + 1) * LANES)
                g, h = ch // 2, ch % 2
                place = ((g % 2) * 2 + g // 2) * 2 + h
                half_gain = 0.5 * gain2[:, cols]
                half_bias = 0.5 * bias2[:, cols]
                for band, average, scale in stats:
                    v = (MX[ch, band, :] - average) * scale * half_gain + half_bias
                    ACT[band, place * LANES : (place + 1) * LANES] = (
                        v + v * jnp.tanh(v)
                    ).astype(jnp.bfloat16)
            band = slice(b * BLK, (b + 1) * BLK)
            lived = lax.broadcasted_iota(jnp.int32, (BLK, wide), 0) < alive_rows[b]
            for s in item_at:

                def side(sy):
                    return jnp.concatenate(
                        [WO[cc, s, sy].reshape(half, LANES) for cc in range(2)], axis=0
                    )

                weights = jnp.concatenate([side(0), side(1)], axis=1)
                o = jnp.dot(ACT[band, :], weights, preferred_element_type=jnp.float32)
                cols = pl.ds(pl.multiple_of(s * wide, wide), wide)
                out[band, cols] = (
                    FR[band, cols].astype(jnp.float32) + jnp.where(lived, o, 0.0)
                ).astype(jnp.bfloat16)

    for token in ORDER:
        arg = [int(d) for d in token if d.isdigit()]
        name = token.rstrip("0123456789")
        if name == "Q":
            own_square(*arg)
        elif name == "R":
            own_line(*arg)
            if arg[0] == 0:
                load.wait()
                halo_start()
                for ch in range(chunks):
                    TP[ch, 0:KER, :] = taps[:, ch * LANES : (ch + 1) * LANES].astype(
                        jnp.float32
                    )
        elif name == "B":
            line(*arg)
        elif name == "XY":
            corner_sends(*arg)
        elif name == "C":
            corner(*arg)
        elif name == "D":
            corner_relay(*arg)
        elif name == "G":
            group(arg[1], arg[0])
        elif name == "P":
            group_partner(arg[1], arg[0])
        elif name == "S":
            column(*arg)
        elif name == "fin":
            finish_all()
        elif name == "halo":
            halo()
        elif not COMPUTE:
            pass
        elif name == "K":
            work(arg)
        elif name == "L":
            work(None)
        elif name == "N":
            norm(*arg)

    if not COMPUTE:
        out[...] = FR[...]

    @pl.when(has_next)
    def _():
        to_next.wait_send()

    @pl.when(has_before)
    def _():
        to_before.wait_send()

    for made in sent:
        made.wait_send()

    @pl.when(end == 0)
    def _():
        for made in middle_sent:
            made.wait_send()


def fused_device(
    frames, ln1_gain, w_in, w_dw, ln2_gain, ln2_bias, w_out, block_utt, block_off, lengths
):
    rows, width = frames.shape
    nz = lax.axis_size("seq") // 2
    krows, _, cols = w_in.shape
    orows, ocols = w_out.shape
    groups = cols // LANES
    wi = w_in.reshape(krows, 2, groups, LANES).transpose(0, 2, 1, 3).reshape(krows, 2 * cols)
    vmem = pl.BlockSpec(memory_space=pltpu.VMEM)
    smem = pl.BlockSpec(memory_space=pltpu.SMEM)
    anywhere = pl.BlockSpec(memory_space=pl.ANY)
    nblk = rows // BLK
    return pl.pallas_call(
        fused_kernel,
        out_shape=jax.ShapeDtypeStruct((rows, width), jnp.bfloat16),
        in_specs=[anywhere] + [vmem] * 6 + [smem] * 3,
        out_specs=vmem,
        scratch_shapes=[
            pltpu.VMEM((2, 2, 2, width, 2 * LANES), jnp.bfloat16),
            pltpu.VMEM((2, nz, 2, 2, orows, ocols), jnp.bfloat16),
            pltpu.VMEM((rows, width), jnp.bfloat16),
            pltpu.VMEM((2, HALO, width), jnp.bfloat16),
            pltpu.VMEM((rows, width), jnp.bfloat16),
            pltpu.VMEM((2 * HALO, width), jnp.bfloat16),
            pltpu.VMEM((nblk * (BLK + 2 * HALO), LANES), jnp.float32),
            pltpu.VMEM((nblk * (BLK + 2 * HALO), LANES), jnp.float32),
            pltpu.VMEM((width // LANES, rows, LANES), jnp.float32),
            pltpu.VMEM((width // LANES, 32, LANES), jnp.float32),
            pltpu.VMEM((rows, width), jnp.bfloat16),
            pltpu.VMEM((rows, LANES), jnp.float32),
            pltpu.VMEM((rows, LANES), jnp.float32),
            pltpu.SMEM((nblk,), jnp.int32),
            pltpu.SMEM((2,), jnp.int32),
            pltpu.SMEM((2,), jnp.float32),
            pltpu.SemaphoreType.DMA((3, KINDS)),
            pltpu.SemaphoreType.DMA((3, KINDS)),
            pltpu.SemaphoreType.DMA((2,)),
            pltpu.SemaphoreType.DMA((2,)),
            pltpu.SemaphoreType.DMA((1,)),
        ],
        compiler_params=pltpu.CompilerParams(
            collective_id=0, has_side_effects=True, vmem_limit_bytes=52 << 20
        ),
    )(
        frames,
        wi,
        w_out,
        ln1_gain[None],
        w_dw,
        ln2_gain[None],
        ln2_bias[None],
        block_utt,
        block_off,
        lengths,
    )


def solution(mesh):
    seq, grp = mesh.shape["seq"], mesh.shape["grp"]
    fits = grp == 4 and seq == 2 * PLANES and D == grp * 2 * LANES

    return jax.shard_map(
        fused_device if fits else per_device,
        mesh=mesh,
        in_specs=(
            P(("seq", "grp"), None),
            P(),
            P("seq", None, "grp"),
            P(),
            P(),
            P(),
            P("grp", "seq"),
            P(),
            P(),
            P(),
        ),
        out_specs=P(("seq", "grp"), None),
        check_vma=False,
    )
```

```python
import functools

import jax
import jax.numpy as jnp
from jax import lax
from jax.experimental import pallas as pl
from jax.experimental.pallas import tpu as pltpu
from jax.sharding import PartitionSpec as P

D = 1024
KER = 31
BLK = 128


epsilon = 1e-05


def extended(block, sides, width):
    for axis, dim in sides:
        count = lax.axis_size(axis)
        forward = [(i, i + 1) for i in range(count - 1)]
        backward = [(target, source) for source, target in forward]
        low = lax.ppermute(
            lax.slice_in_dim(block, block.shape[dim] - width, None, axis=dim), axis, forward
        )
        high = lax.ppermute(lax.slice_in_dim(block, 0, width, axis=dim), axis, backward)
        block = jnp.concatenate([low, block, high], axis=dim)
    return block


def frame_keys(block_utt, block_off, lengths, first_row, row_count, margin):
    places = first_row - margin + jnp.arange(row_count + 2 * margin, dtype=jnp.int32)
    total_rows = block_utt.shape[0] * BLK
    inside = (places >= 0) & (places < total_rows)
    blocks = jnp.clip(places // BLK, 0, block_utt.shape[0] - 1)
    utterance = jnp.take(block_utt, blocks)
    position = jnp.take(block_off, blocks) * BLK + places % BLK
    living = inside & (position < jnp.take(lengths, utterance))
    return (jnp.where(living, utterance, -1), living[margin : margin + row_count])


def layer_norm(rows, gain):
    values = rows.astype(jnp.float32)
    average = jnp.mean(values, axis=1, keepdims=True)
    centered = values - average
    spread = jnp.mean(centered * centered, axis=1, keepdims=True)
    return (centered * lax.rsqrt(spread + epsilon) * gain).astype(jnp.bfloat16)


def gate_units(projected, living):
    half = projected.shape[1] // 2
    values = projected[:, :half] * jax.nn.sigmoid(projected[:, half:])
    return (values * living.astype(jnp.float32)[:, None]).astype(jnp.bfloat16)


def depthwise(widened, keys_wide, taps, row_count):
    margin = (taps.shape[0] - 1) // 2
    center = keys_wide[margin : margin + row_count]
    summed = jnp.zeros((row_count, widened.shape[1]), jnp.float32)
    for tap_index in range(taps.shape[0]):
        shifted = widened[tap_index : tap_index + row_count].astype(jnp.float32)
        same = (keys_wide[tap_index : tap_index + row_count] == center)[:, None]
        summed = summed + jnp.where(same, shifted, 0.0) * taps[tap_index].astype(jnp.float32)
    return summed


def finish(mixed, stat_sum, square_sum, width_total, gain, bias):
    average = stat_sum / width_total
    spread = square_sum / width_total - average * average
    normed = (mixed - average[:, None]) * lax.rsqrt(spread + epsilon)[:, None] * gain + bias
    return (normed * jax.nn.sigmoid(normed)).astype(jnp.bfloat16)


def project_rows(normed, row_count, column_count):

    def add_rows(total, weight_piece, start_row):
        piece_rows = weight_piece.shape[0]
        return jnp.dot(
            normed, weight_piece.reshape(piece_rows, -1), preferred_element_type=jnp.float32
        )

    return (add_rows, jnp.zeros((row_count, column_count), jnp.float32))


def per_device(
    frames, ln1_gain, w_in, w_dw, ln2_gain, ln2_bias, w_out, block_utt, block_off, lengths
):
    row_count = frames.shape[0]
    margin = (KER - 1) // 2
    own_first = lax.axis_index(("seq", "grp")) * row_count
    keys_wide, living = frame_keys(block_utt, block_off, lengths, own_first, row_count, margin)
    normed = layer_norm(frames, ln1_gain)
    w_in_rows, w_out_rows = (
        lax.all_gather(w_in, "grp", axis=2, tiled=True),
        lax.all_gather(w_out, "grp", axis=0, tiled=True),
    )
    add_rows, empty = project_rows(normed, row_count, 2 * D)
    projected = add_rows(empty, lax.all_gather(w_in_rows, "seq", axis=0, tiled=True), jnp.int32(0))
    gated = gate_units(projected, living)
    widened = extended(gated, ((("seq", "grp"), 0),), margin)
    mixed = depthwise(widened, keys_wide, w_dw, row_count)
    act = finish(
        mixed, jnp.sum(mixed, axis=1), jnp.sum(mixed * mixed, axis=1), float(D), ln2_gain, ln2_bias
    )
    output = jnp.dot(
        act,
        lax.all_gather(w_out_rows, "seq", axis=1, tiled=True),
        preferred_element_type=jnp.float32,
    )
    alive = living.astype(jnp.float32)[:, None]
    return (frames.astype(jnp.float32) + output * alive).astype(jnp.bfloat16)


MESH = pl.DeviceIdType.MESH
HALO = 16
LANES = 128
PLANES = 4
O, X, Y, CX, CY, CZ, PP = (PLANES * i for i in range(7))
KINDS = 7 * PLANES + 8
COMPUTE = True

ORDER = (
    "Q0", "R0", "Q1", "N0", "XY00", "B00", "R1", "B01", "N1", "C00",
    "XY10", "Q2", "XY01", "B02", "B10", "B11", "R2", "C10", "C01", "D0",
    "G00", "halo", "K000", "XY20", "B20", "XY11", "B12", "L0", "P00", "G10",
    "K010", "C20", "B21", "C11", "D1", "L1", "G01", "K001", "XY21", "B22",
    "P10", "K100", "G11", "C21", "D2", "P01", "K011", "S0", "S1", "S2",
    "K110", "P11", "S3", "K101", "K111", "L3", "fin",
)


def fused_kernel(
    frames_hbm,
    wi_own,
    wo_own,
    gain1,
    taps,
    gain2,
    bias2,
    utts,
    offs,
    lens,
    out,
    WI,
    WO,
    FR,
    HB,
    NM,
    NH,
    GB0,
    GB1,
    MX,
    TP,
    ACT,
    S1,
    S2,
    limits,
    edge_limits,
    edge_joined,
    ssem,
    rsem,
    hs,
    hr,
    lsem,
):
    rows, width = FR.shape
    krows = wi_own.shape[0]
    nblk = rows // BLK
    chunks = width // LANES
    seq = lax.axis_index("seq")
    grp = lax.axis_index("grp")
    nseq = lax.axis_size("seq")
    ngrp = lax.axis_size("grp")
    z, y = seq // 2, seq % 2
    x, c = grp // 2, grp % 2
    index = seq * ngrp + grp
    total = nseq * ngrp
    hi, lo = z // 2, z % 2
    end = 1 - hi - lo + 2 * hi * lo
    near = 2 * hi + 1 - lo
    item_at = (z, 3 - z, near, 3 - near)
    source_at = (
        end * near + (1 - end) * (3 - z),
        end * (3 - z) + (1 - end) * near,
        3 - near,
    )

    px = (seq, (1 - x) * 2 + c)
    py = (z * 2 + 1 - y, grp)
    pp = (seq, x * 2 + 1 - c)
    has_next = index < total - 1
    has_before = index > 0
    after = jnp.minimum(index + 1, total - 1)
    before = jnp.maximum(index - 1, 0)
    pn = (after // ngrp, after % ngrp)
    pb = (before // ngrp, before % ngrp)

    def plane(t):
        return (t * 2 + y, grp)

    load = pltpu.make_async_copy(frames_hbm, FR, lsem.at[0])
    load.start()

    barrier = pltpu.get_barrier_semaphore()
    peers = [px, py, pp] + [plane((z + k) % PLANES) for k in range(1, PLANES)]
    for peer in peers:
        pl.semaphore_signal(barrier, inc=1, device_id=peer, device_id_type=MESH)

    @pl.when(has_next)
    def _():
        pl.semaphore_signal(barrier, inc=1, device_id=pn, device_id_type=MESH)

    @pl.when(has_before)
    def _():
        pl.semaphore_signal(barrier, inc=1, device_id=pb, device_id_type=MESH)

    @pl.when(jnp.logical_not(has_before))
    def _():
        HB[0] = jnp.zeros((HALO, width), jnp.bfloat16)

    @pl.when(jnp.logical_not(has_next))
    def _():
        HB[1] = jnp.zeros((HALO, width), jnp.bfloat16)

    own_rows = pl.ds(pl.multiple_of(seq * krows, krows), krows)
    for h in range(2):
        WI[h, c, x, own_rows, :] = wi_own[:, h * 2 * LANES : (h + 1) * 2 * LANES]
    WO[c, z, y, x] = wo_own[...]
    pl.semaphore_wait(
        barrier, len(peers) + has_next.astype(jnp.int32) + has_before.astype(jnp.int32)
    )

    def slot(w, sx, sy, sz, half=None):
        if w < 2:
            count = krows if half is None else krows // 2
            first = (sz * 2 + sy) * krows + (0 if half is None else half * count)
            return WI.at[w, c, sx, pl.ds(pl.multiple_of(first, count), count), :]
        if half is None:
            return WO.at[c, sz, sy, sx]
        count = WO.shape[4] // 2
        return WO.at[c, sz, sy, sx, pl.ds(half * count, count), :]

    sent = []
    middle_sent = []

    def copy(w, ref, sem, dev):
        return pltpu.make_async_remote_copy(
            src_ref=ref,
            dst_ref=ref,
            send_sem=ssem.at[w, len(sent) % KINDS],
            recv_sem=rsem.at[w, sem],
            device_id=dev,
            device_id_type=MESH,
        )

    count_of = [0, 0, 0]

    def send(w, ref, sem, dev):
        made = pltpu.make_async_remote_copy(
            src_ref=ref,
            dst_ref=ref,
            send_sem=ssem.at[w, count_of[w]],
            recv_sem=rsem.at[w, sem],
            device_id=dev,
            device_id_type=MESH,
        )
        made.start()
        count_of[w] += 1
        sent.append(made)

    def receive(w, ref, sem):
        copy(w, ref, sem, px).wait_recv()

    def middle_send(w, ref, sem, dev):
        made = pltpu.make_async_remote_copy(
            src_ref=ref,
            dst_ref=ref,
            send_sem=ssem.at[w, count_of[w]],
            recv_sem=rsem.at[w, sem],
            device_id=dev,
            device_id_type=MESH,
        )
        count_of[w] += 1
        middle_sent.append(made)

        @pl.when(end == 0)
        def _():
            made.start()

    def own_square(w):
        ref = slot(w, x, y, z)
        send(w, ref, X + z, px)
        send(w, ref, Y + z, py)

    def own_line(w):
        ref = slot(w, x, y, z)
        send(w, ref, O + z, plane(3 - z))
        send(w, ref, O + z, plane(near))

    def line(w, p):
        s = source_at[p]
        ref = slot(w, x, y, s)
        receive(w, ref, O + s)
        if p == 0:
            middle_send(w, slot(w, x, y, 3 - z), O + 3 - z, plane(near))
        if p == 1:
            middle_send(w, slot(w, x, y, near), O + near, plane(3 - z))
        send(w, ref, X + s, px)
        send(w, ref, Y + s, py)

    def corner_relay(w):
        ref = slot(w, 1 - x, 1 - y, near)
        receive(w, ref, CZ + near)
        middle_send(w, ref, CZ + near, plane(3 - z))

    def corner_sends(w, i):
        s = item_at[i]
        receive(w, slot(w, x, 1 - y, s), Y + s)
        send(w, slot(w, x, 1 - y, s, 0), CX + s, px)
        receive(w, slot(w, 1 - x, y, s), X + s)
        send(w, slot(w, 1 - x, y, s, 1), CY + s, py)

    def corner(w, i):
        s = item_at[i]
        receive(w, slot(w, 1 - x, 1 - y, s, 0), CX + s)
        receive(w, slot(w, 1 - x, 1 - y, s, 1), CY + s)
        if i == 0:
            send(w, slot(w, 1 - x, 1 - y, s), CZ + s, plane(near))
        else:
            middle_send(w, slot(w, 1 - x, 1 - y, s), CZ + s, plane(near))

    def group(w, rel):
        if rel == 0:
            for s in item_at[2:]:
                receive(w, slot(w, x, 1 - y, s), Y + s)
            send(w, WI.at[w, c, x], PP, pp)
        else:
            for s in item_at[2:]:
                receive(w, slot(w, 1 - x, y, s), X + s)
            receive(w, slot(w, 1 - x, 1 - y, 3 - near), CZ + 3 - near)
            send(w, WI.at[w, c, 1 - x], PP + 1, pp)

    def group_partner(w, rel):
        receive(w, WI.at[w, 1 - c, x if rel == 0 else 1 - x], PP + rel)

    def column(i):
        s = item_at[i]
        if i >= 2:
            receive(2, slot(2, x, 1 - y, s), Y + s)
            receive(2, slot(2, 1 - x, y, s), X + s)
        if i == 3:
            receive(2, slot(2, 1 - x, 1 - y, s), CZ + s)
        send(2, WO.at[c, s], PP + s, pp)

    def halo_copy(src, dst, sem, dev):
        return pltpu.make_async_remote_copy(
            src_ref=src,
            dst_ref=dst,
            send_sem=hs.at[sem],
            recv_sem=hr.at[sem],
            device_id=dev,
            device_id_type=MESH,
        )

    to_next = halo_copy(FR.at[pl.ds(rows - HALO, HALO), :], HB.at[0], 0, pn)
    to_before = halo_copy(FR.at[pl.ds(0, HALO), :], HB.at[1], 1, pb)

    def halo_start():
        @pl.when(has_next)
        def _():
            to_next.start()

        @pl.when(has_before)
        def _():
            to_before.start()

    def norm_rows(block):
        values = block.astype(jnp.float32)
        average = jnp.mean(values, axis=1, keepdims=True)
        centered = values - average
        spread_ = jnp.mean(centered * centered, axis=1, keepdims=True)
        return (centered * lax.rsqrt(spread_ + epsilon) * gain1[...]).astype(jnp.bfloat16)

    tall_rows = BLK
    pack = 2 * 8

    def tile(ref, first, ch):
        return ref[pl.ds(first, pack), ch * LANES : (ch + 1) * LANES].astype(jnp.float32)

    def row_sum(parts):
        total_ = parts[0]
        for part in parts[1:]:
            total_ = total_ + part
        return jnp.sum(total_, axis=1, keepdims=True)

    def norm(step):
        def bands(i):
            return [
                pl.multiple_of(i * tall_rows + r * pack, pack) for r in range(tall_rows // pack)
            ]

        def average_step(i, carry):
            for first in bands(i):
                average = row_sum([tile(FR, first, ch) for ch in range(chunks)]) / float(width)
                S1[pl.ds(first, pack), :] = jnp.broadcast_to(average, (pack, LANES))
            return carry

        def spread_step(i, carry):
            for first in bands(i):
                average = S1[pl.ds(first, pack), :]
                parts = [tile(FR, first, ch) - average for ch in range(chunks)]
                spread = row_sum([p * p for p in parts]) / float(width)
                scale = lax.rsqrt(spread + epsilon)
                S2[pl.ds(first, pack), :] = jnp.broadcast_to(scale, (pack, LANES))
            return carry

        def scale_step(i, carry):
            for first in bands(i):
                average = S1[pl.ds(first, pack), :]
                scale = S2[pl.ds(first, pack), :]
                for ch in range(chunks):
                    cols = slice(ch * LANES, (ch + 1) * LANES)
                    NM[pl.ds(first, pack), cols] = (
                        (tile(FR, first, ch) - average) * scale * gain1[:, cols]
                    ).astype(jnp.bfloat16)
            return carry

        count = rows // tall_rows // 2
        for stage in (average_step, spread_step, scale_step):
            lax.fori_loop(count * step, count * (step + 1), stage, 0)

    def halo():
        @pl.when(has_before)
        def _():
            to_next.wait_recv()

        @pl.when(has_next)
        def _():
            to_before.wait_recv()

        NH[0:HALO, :] = norm_rows(HB[0])
        NH[HALO:, :] = norm_rows(HB[1])

    first_block = index * nblk
    last_block = total * nblk - 1

    def block_info(b):
        u = utts[b]
        return u, lens[u] - offs[b] * BLK

    info = [
        block_info(jnp.clip(first_block + i, 0, last_block)) for i in range(-1, nblk + 1)
    ]
    joined = []
    for i in range(nblk + 1):
        same = info[i][0] == info[i + 1][0]
        if i == 0:
            same = same & (first_block > 0)
        if i == nblk:
            same = same & (first_block + nblk <= last_block)
        joined.append(same.astype(jnp.float32))
    alive_rows = [info[i + 1][1] for i in range(nblk)]
    for i in range(nblk):
        limits[i] = alive_rows[i]
    edge_limits[0] = info[0][1] - (BLK - HALO)
    edge_limits[1] = info[nblk + 1][1]
    edge_joined[0] = joined[0]
    edge_joined[1] = joined[nblk]

    def tall(count, start):
        return start + lax.broadcasted_iota(jnp.int32, (count, LANES), 0)

    stride = BLK + 2 * HALO

    def chunk_of(h, rel_c, rel_x):
        cc = c if rel_c == 0 else 1 - c
        xx = x if rel_x == 0 else 1 - x
        return cc, xx, (xx * 2 + cc) * 2 + h

    started = []
    pending = []
    deep = 4
    part_rows = 16 * deep
    parts = BLK // part_rows

    def convolve_step(j, ch, buf, fresh, tap):
        i, q = j // (2 * parts), j % (2 * parts)
        base = pl.multiple_of(i * stride + q * (8 * deep), 8)
        sums = [None] * deep
        for o in range(8 * (deep - 1) + KER):
            value = buf[pl.ds(base + (1 + o), 8), :]
            for t in range(deep):
                k = o - 8 * t
                if 0 <= k < KER:
                    term = value * tap[k]
                    sums[t] = term if sums[t] is None else sums[t] + term
        first = pl.multiple_of(j * (8 * deep), 8 * deep)
        for t in range(deep):
            band = pl.ds(pl.multiple_of(first + 8 * t, 8), 8)
            MX[ch, band, :] = sums[t]
            if fresh:
                S1[band, :] = sums[t]
                S2[band, :] = sums[t] * sums[t]
            else:
                S1[band, :] += sums[t]
                S2[band, :] += sums[t] * sums[t]

    def work(project_id):
        earlier = pending.pop() if pending else None
        if earlier is None and project_id is None:
            return
        if earlier is not None:
            old_ch, old_buf, fresh = earlier
            tap = [jnp.broadcast_to(TP[old_ch, k : k + 1, :], (8, LANES)) for k in range(KER)]
        if project_id is not None:
            h = project_id[0]
            cc, xx, ch = chunk_of(*project_id)
            buf = (GB0, GB1)[len(started) % 2]
            pending.append((ch, buf, not started))
            started.append(ch)

        def gated(p):
            half = 0.5 * p[:, :LANES]
            return half + half * jnp.tanh(0.5 * p[:, LANES:])

        def rounded(units):
            return units.astype(jnp.bfloat16).astype(jnp.float32)

        def at_once(between):
            lhs = jnp.concatenate([NM[...], NH[...]], axis=0)
            p = jnp.dot(lhs, WI[h, cc, xx], preferred_element_type=jnp.float32)
            between()
            units = gated(p)
            for i in range(nblk):
                main = jnp.where(tall(BLK, 0) < alive_rows[i], units[i * BLK : (i + 1) * BLK], 0.0)
                buf[i * stride + HALO : i * stride + HALO + BLK, :] = rounded(main)
            for q in range(2):
                strip = units[rows + q * HALO : rows + (q + 1) * HALO]
                strip = rounded(jnp.where(tall(HALO, 0) < edge_limits[q], strip, 0.0))
                place = q * (nblk * stride - HALO)
                buf[place : place + HALO, :] = strip * edge_joined[q]

        def convolve(steps):
            for j in steps:
                convolve_step(j, old_ch, old_buf, fresh, tap)

        count = 2 * nblk * parts
        if earlier is None:
            at_once(lambda: None)
        elif project_id is None:

            def step(j, carry):
                convolve((2 * j, 2 * j + 1))
                return carry

            lax.fori_loop(0, count // 2, step, 0)
        else:
            at_once(lambda: convolve(range(count)))
        if project_id is not None:
            for i in range(1, nblk):
                base = i * stride
                buf[base : base + HALO, :] = (
                    buf[base - 2 * HALO : base - HALO, :] * joined[i]
                )
                buf[base - HALO : base, :] = (
                    buf[base + HALO : base + 2 * HALO, :] * joined[i]
                )

    wide = 2 * LANES

    def finish_all():
        half = WO.shape[3] * WO.shape[4]
        for s in item_at:
            receive(2, WO.at[1 - c, s], PP + s)
        if not COMPUTE:
            return
        for b in range(nblk):
            stats = []
            for r in range(tall_rows // pack):
                band = slice(b * BLK + r * pack, b * BLK + (r + 1) * pack)
                average = jnp.sum(S1[band, :], axis=1, keepdims=True) / float(width)
                square = jnp.sum(S2[band, :], axis=1, keepdims=True) / float(width)
                scale = lax.rsqrt(square - average * average + epsilon)
                stats.append((band, average, scale))
            for ch in range(chunks):
                cols = slice(ch * LANES, (ch + 1) * LANES)
                g, h = ch // 2, ch % 2
                place = ((g % 2) * 2 + g // 2) * 2 + h
                half_gain = 0.5 * gain2[:, cols]
                half_bias = 0.5 * bias2[:, cols]
                for band, average, scale in stats:
                    v = (MX[ch, band, :] - average) * scale * half_gain + half_bias
                    ACT[band, place * LANES : (place + 1) * LANES] = (
                        v + v * jnp.tanh(v)
                    ).astype(jnp.bfloat16)
            band = slice(b * BLK, (b + 1) * BLK)
            lived = lax.broadcasted_iota(jnp.int32, (BLK, wide), 0) < alive_rows[b]
            for s in item_at:

                def side(sy):
                    return jnp.concatenate(
                        [WO[cc, s, sy].reshape(half, LANES) for cc in range(2)], axis=0
                    )

                weights = jnp.concatenate([side(0), side(1)], axis=1)
                o = jnp.dot(ACT[band, :], weights, preferred_element_type=jnp.float32)
                cols = pl.ds(pl.multiple_of(s * wide, wide), wide)
                out[band, cols] = (
                    FR[band, cols].astype(jnp.float32) + jnp.where(lived, o, 0.0)
                ).astype(jnp.bfloat16)

    for token in ORDER:
        arg = [int(d) for d in token if d.isdigit()]
        name = token.rstrip("0123456789")
        if name == "Q":
            own_square(*arg)
        elif name == "R":
            own_line(*arg)
            if arg[0] == 0:
                load.wait()
                halo_start()
                for ch in range(chunks):
                    TP[ch, 0:KER, :] = taps[:, ch * LANES : (ch + 1) * LANES].astype(
                        jnp.float32
                    )
        elif name == "B":
            line(*arg)
        elif name == "XY":
            corner_sends(*arg)
        elif name == "C":
            corner(*arg)
        elif name == "D":
            corner_relay(*arg)
        elif name == "G":
            group(arg[1], arg[0])
        elif name == "P":
            group_partner(arg[1], arg[0])
        elif name == "S":
            column(*arg)
        elif name == "fin":
            finish_all()
        elif name == "halo":
            halo()
        elif not COMPUTE:
            pass
        elif name == "K":
            work(arg)
        elif name == "L":
            work(None)
        elif name == "N":
            norm(*arg)

    if not COMPUTE:
        out[...] = FR[...]

    @pl.when(has_next)
    def _():
        to_next.wait_send()

    @pl.when(has_before)
    def _():
        to_before.wait_send()

    for made in sent:
        made.wait_send()

    @pl.when(end == 0)
    def _():
        for made in middle_sent:
            made.wait_send()


def fused_device(
    frames, ln1_gain, w_in, w_dw, ln2_gain, ln2_bias, w_out, block_utt, block_off, lengths
):
    rows, width = frames.shape
    nz = lax.axis_size("seq") // 2
    krows, _, cols = w_in.shape
    orows, ocols = w_out.shape
    groups = cols // LANES
    wi = w_in.reshape(krows, 2, groups, LANES).transpose(0, 2, 1, 3).reshape(krows, 2 * cols)
    vmem = pl.BlockSpec(memory_space=pltpu.VMEM)
    smem = pl.BlockSpec(memory_space=pltpu.SMEM)
    anywhere = pl.BlockSpec(memory_space=pl.ANY)
    nblk = rows // BLK
    return pl.pallas_call(
        fused_kernel,
        out_shape=jax.ShapeDtypeStruct((rows, width), jnp.bfloat16),
        in_specs=[anywhere] + [vmem] * 6 + [smem] * 3,
        out_specs=vmem,
        scratch_shapes=[
            pltpu.VMEM((2, 2, 2, width, 2 * LANES), jnp.bfloat16),
            pltpu.VMEM((2, nz, 2, 2, orows, ocols), jnp.bfloat16),
            pltpu.VMEM((rows, width), jnp.bfloat16),
            pltpu.VMEM((2, HALO, width), jnp.bfloat16),
            pltpu.VMEM((rows, width), jnp.bfloat16),
            pltpu.VMEM((2 * HALO, width), jnp.bfloat16),
            pltpu.VMEM((nblk * (BLK + 2 * HALO), LANES), jnp.float32),
            pltpu.VMEM((nblk * (BLK + 2 * HALO), LANES), jnp.float32),
            pltpu.VMEM((width // LANES, rows, LANES), jnp.float32),
            pltpu.VMEM((width // LANES, 32, LANES), jnp.float32),
            pltpu.VMEM((rows, width), jnp.bfloat16),
            pltpu.VMEM((rows, LANES), jnp.float32),
            pltpu.VMEM((rows, LANES), jnp.float32),
            pltpu.SMEM((nblk,), jnp.int32),
            pltpu.SMEM((2,), jnp.int32),
            pltpu.SMEM((2,), jnp.float32),
            pltpu.SemaphoreType.DMA((3, KINDS)),
            pltpu.SemaphoreType.DMA((3, KINDS)),
            pltpu.SemaphoreType.DMA((2,)),
            pltpu.SemaphoreType.DMA((2,)),
            pltpu.SemaphoreType.DMA((1,)),
        ],
        compiler_params=pltpu.CompilerParams(
            collective_id=0, has_side_effects=True, vmem_limit_bytes=52 << 20
        ),
    )(
        frames,
        wi,
        w_out,
        ln1_gain[None],
        w_dw,
        ln2_gain[None],
        ln2_bias[None],
        block_utt,
        block_off,
        lengths,
    )


def solution(mesh):
    seq, grp = mesh.shape["seq"], mesh.shape["grp"]
    fits = grp == 4 and seq == 2 * PLANES and D == grp * 2 * LANES

    return jax.shard_map(
        fused_device if fits else per_device,
        mesh=mesh,
        in_specs=(
            P(("seq", "grp"), None),
            P(),
            P("seq", None, "grp"),
            P(),
            P(),
            P(),
            P("grp", "seq"),
            P(),
            P(),
            P(),
        ),
        out_specs=P(("seq", "grp"), None),
        check_vma=False,
    )
```

```python
import functools

import jax
import jax.numpy as jnp
from jax import lax
from jax.experimental import pallas as pl
from jax.experimental.pallas import tpu as pltpu
from jax.sharding import PartitionSpec as P

D = 1024
KER = 31
BLK = 128


epsilon = 1e-05


def extended(block, sides, width):
    for axis, dim in sides:
        count = lax.axis_size(axis)
        forward = [(i, i + 1) for i in range(count - 1)]
        backward = [(target, source) for source, target in forward]
        low = lax.ppermute(
            lax.slice_in_dim(block, block.shape[dim] - width, None, axis=dim), axis, forward
        )
        high = lax.ppermute(lax.slice_in_dim(block, 0, width, axis=dim), axis, backward)
        block = jnp.concatenate([low, block, high], axis=dim)
    return block


def frame_keys(block_utt, block_off, lengths, first_row, row_count, margin):
    places = first_row - margin + jnp.arange(row_count + 2 * margin, dtype=jnp.int32)
    total_rows = block_utt.shape[0] * BLK
    inside = (places >= 0) & (places < total_rows)
    blocks = jnp.clip(places // BLK, 0, block_utt.shape[0] - 1)
    utterance = jnp.take(block_utt, blocks)
    position = jnp.take(block_off, blocks) * BLK + places % BLK
    living = inside & (position < jnp.take(lengths, utterance))
    return (jnp.where(living, utterance, -1), living[margin : margin + row_count])


def layer_norm(rows, gain):
    values = rows.astype(jnp.float32)
    average = jnp.mean(values, axis=1, keepdims=True)
    centered = values - average
    spread = jnp.mean(centered * centered, axis=1, keepdims=True)
    return (centered * lax.rsqrt(spread + epsilon) * gain).astype(jnp.bfloat16)


def gate_units(projected, living):
    half = projected.shape[1] // 2
    values = projected[:, :half] * jax.nn.sigmoid(projected[:, half:])
    return (values * living.astype(jnp.float32)[:, None]).astype(jnp.bfloat16)


def depthwise(widened, keys_wide, taps, row_count):
    margin = (taps.shape[0] - 1) // 2
    center = keys_wide[margin : margin + row_count]
    summed = jnp.zeros((row_count, widened.shape[1]), jnp.float32)
    for tap_index in range(taps.shape[0]):
        shifted = widened[tap_index : tap_index + row_count].astype(jnp.float32)
        same = (keys_wide[tap_index : tap_index + row_count] == center)[:, None]
        summed = summed + jnp.where(same, shifted, 0.0) * taps[tap_index].astype(jnp.float32)
    return summed


def finish(mixed, stat_sum, square_sum, width_total, gain, bias):
    average = stat_sum / width_total
    spread = square_sum / width_total - average * average
    normed = (mixed - average[:, None]) * lax.rsqrt(spread + epsilon)[:, None] * gain + bias
    return (normed * jax.nn.sigmoid(normed)).astype(jnp.bfloat16)


def project_rows(normed, row_count, column_count):

    def add_rows(total, weight_piece, start_row):
        piece_rows = weight_piece.shape[0]
        return jnp.dot(
            normed, weight_piece.reshape(piece_rows, -1), preferred_element_type=jnp.float32
        )

    return (add_rows, jnp.zeros((row_count, column_count), jnp.float32))


def per_device(
    frames, ln1_gain, w_in, w_dw, ln2_gain, ln2_bias, w_out, block_utt, block_off, lengths
):
    row_count = frames.shape[0]
    margin = (KER - 1) // 2
    own_first = lax.axis_index(("seq", "grp")) * row_count
    keys_wide, living = frame_keys(block_utt, block_off, lengths, own_first, row_count, margin)
    normed = layer_norm(frames, ln1_gain)
    w_in_rows, w_out_rows = (
        lax.all_gather(w_in, "grp", axis=2, tiled=True),
        lax.all_gather(w_out, "grp", axis=0, tiled=True),
    )
    add_rows, empty = project_rows(normed, row_count, 2 * D)
    projected = add_rows(empty, lax.all_gather(w_in_rows, "seq", axis=0, tiled=True), jnp.int32(0))
    gated = gate_units(projected, living)
    widened = extended(gated, ((("seq", "grp"), 0),), margin)
    mixed = depthwise(widened, keys_wide, w_dw, row_count)
    act = finish(
        mixed, jnp.sum(mixed, axis=1), jnp.sum(mixed * mixed, axis=1), float(D), ln2_gain, ln2_bias
    )
    output = jnp.dot(
        act,
        lax.all_gather(w_out_rows, "seq", axis=1, tiled=True),
        preferred_element_type=jnp.float32,
    )
    alive = living.astype(jnp.float32)[:, None]
    return (frames.astype(jnp.float32) + output * alive).astype(jnp.bfloat16)


MESH = pl.DeviceIdType.MESH
HALO = 16
LANES = 128
PLANES = 4
O, X, Y, CX, CY, CZ, PP = (PLANES * i for i in range(7))
KINDS = 7 * PLANES + 8
COMPUTE = True

ORDER = (
    "Q0", "R0", "Q1", "N0", "XY00", "B00", "R1", "B01", "N1", "C00",
    "XY10", "Q2", "XY01", "B02", "B10", "B11", "R2", "C10", "C01", "D0",
    "G00", "halo", "K000", "XY20", "B20", "XY11", "B12", "L0", "P00", "G10",
    "K010", "C20", "B21", "L1", "C11", "D1", "G01", "K001", "XY21", "B22",
    "P10", "K100", "G11", "K011", "C21", "D2", "P01", "S0", "S1", "S2",
    "K110", "K101", "S3", "P11", "K111", "L3", "fin",
)


def fused_kernel(
    frames_hbm,
    wi_own,
    wo_own,
    gain1,
    taps,
    gain2,
    bias2,
    utts,
    offs,
    lens,
    out,
    WI,
    WO,
    FR,
    HB,
    NM,
    NH,
    GB0,
    GB1,
    MX,
    TP,
    ACT,
    S1,
    S2,
    limits,
    edge_limits,
    edge_joined,
    ssem,
    rsem,
    hs,
    hr,
    lsem,
):
    rows, width = FR.shape
    krows = wi_own.shape[0]
    nblk = rows // BLK
    chunks = width // LANES
    seq = lax.axis_index("seq")
    grp = lax.axis_index("grp")
    nseq = lax.axis_size("seq")
    ngrp = lax.axis_size("grp")
    z, y = seq // 2, seq % 2
    x, c = grp // 2, grp % 2
    index = seq * ngrp + grp
    total = nseq * ngrp
    hi, lo = z // 2, z % 2
    end = 1 - hi - lo + 2 * hi * lo
    near = 2 * hi + 1 - lo
    item_at = (z, 3 - z, near, 3 - near)
    source_at = (
        end * near + (1 - end) * (3 - z),
        end * (3 - z) + (1 - end) * near,
        3 - near,
    )

    px = (seq, (1 - x) * 2 + c)
    py = (z * 2 + 1 - y, grp)
    pp = (seq, x * 2 + 1 - c)
    has_next = index < total - 1
    has_before = index > 0
    after = jnp.minimum(index + 1, total - 1)
    before = jnp.maximum(index - 1, 0)
    pn = (after // ngrp, after % ngrp)
    pb = (before // ngrp, before % ngrp)

    def plane(t):
        return (t * 2 + y, grp)

    load = pltpu.make_async_copy(frames_hbm, FR, lsem.at[0])
    load.start()

    barrier = pltpu.get_barrier_semaphore()
    peers = [px, py, pp] + [plane((z + k) % PLANES) for k in range(1, PLANES)]
    for peer in peers:
        pl.semaphore_signal(barrier, inc=1, device_id=peer, device_id_type=MESH)

    @pl.when(has_next)
    def _():
        pl.semaphore_signal(barrier, inc=1, device_id=pn, device_id_type=MESH)

    @pl.when(has_before)
    def _():
        pl.semaphore_signal(barrier, inc=1, device_id=pb, device_id_type=MESH)

    @pl.when(jnp.logical_not(has_before))
    def _():
        HB[0] = jnp.zeros((HALO, width), jnp.bfloat16)

    @pl.when(jnp.logical_not(has_next))
    def _():
        HB[1] = jnp.zeros((HALO, width), jnp.bfloat16)

    own_rows = pl.ds(pl.multiple_of(seq * krows, krows), krows)
    for h in range(2):
        WI[h, c, x, own_rows, :] = wi_own[:, h * 2 * LANES : (h + 1) * 2 * LANES]
    WO[c, z, y, x] = wo_own[...]
    pl.semaphore_wait(
        barrier, len(peers) + has_next.astype(jnp.int32) + has_before.astype(jnp.int32)
    )

    def slot(w, sx, sy, sz, half=None):
        if w < 2:
            count = krows if half is None else krows // 2
            first = (sz * 2 + sy) * krows + (0 if half is None else half * count)
            return WI.at[w, c, sx, pl.ds(pl.multiple_of(first, count), count), :]
        if half is None:
            return WO.at[c, sz, sy, sx]
        count = WO.shape[4] // 2
        return WO.at[c, sz, sy, sx, pl.ds(half * count, count), :]

    sent = []
    middle_sent = []

    def copy(w, ref, sem, dev):
        return pltpu.make_async_remote_copy(
            src_ref=ref,
            dst_ref=ref,
            send_sem=ssem.at[w, len(sent) % KINDS],
            recv_sem=rsem.at[w, sem],
            device_id=dev,
            device_id_type=MESH,
        )

    count_of = [0, 0, 0]

    def send(w, ref, sem, dev):
        made = pltpu.make_async_remote_copy(
            src_ref=ref,
            dst_ref=ref,
            send_sem=ssem.at[w, count_of[w]],
            recv_sem=rsem.at[w, sem],
            device_id=dev,
            device_id_type=MESH,
        )
        made.start()
        count_of[w] += 1
        sent.append(made)

    def receive(w, ref, sem):
        copy(w, ref, sem, px).wait_recv()

    def middle_send(w, ref, sem, dev):
        made = pltpu.make_async_remote_copy(
            src_ref=ref,
            dst_ref=ref,
            send_sem=ssem.at[w, count_of[w]],
            recv_sem=rsem.at[w, sem],
            device_id=dev,
            device_id_type=MESH,
        )
        count_of[w] += 1
        middle_sent.append(made)

        @pl.when(end == 0)
        def _():
            made.start()

    def own_square(w):
        ref = slot(w, x, y, z)
        send(w, ref, X + z, px)
        send(w, ref, Y + z, py)

    def own_line(w):
        ref = slot(w, x, y, z)
        send(w, ref, O + z, plane(3 - z))
        send(w, ref, O + z, plane(near))

    def line(w, p):
        s = source_at[p]
        ref = slot(w, x, y, s)
        receive(w, ref, O + s)
        if p == 0:
            middle_send(w, slot(w, x, y, 3 - z), O + 3 - z, plane(near))
        if p == 1:
            middle_send(w, slot(w, x, y, near), O + near, plane(3 - z))
        send(w, ref, X + s, px)
        send(w, ref, Y + s, py)

    def corner_relay(w):
        ref = slot(w, 1 - x, 1 - y, near)
        receive(w, ref, CZ + near)
        middle_send(w, ref, CZ + near, plane(3 - z))

    def corner_sends(w, i):
        s = item_at[i]
        receive(w, slot(w, x, 1 - y, s), Y + s)
        send(w, slot(w, x, 1 - y, s, 0), CX + s, px)
        receive(w, slot(w, 1 - x, y, s), X + s)
        send(w, slot(w, 1 - x, y, s, 1), CY + s, py)

    def corner(w, i):
        s = item_at[i]
        receive(w, slot(w, 1 - x, 1 - y, s, 0), CX + s)
        receive(w, slot(w, 1 - x, 1 - y, s, 1), CY + s)
        if i == 0:
            send(w, slot(w, 1 - x, 1 - y, s), CZ + s, plane(near))
        else:
            middle_send(w, slot(w, 1 - x, 1 - y, s), CZ + s, plane(near))

    def group(w, rel):
        if rel == 0:
            for s in item_at[2:]:
                receive(w, slot(w, x, 1 - y, s), Y + s)
            send(w, WI.at[w, c, x], PP, pp)
        else:
            for s in item_at[2:]:
                receive(w, slot(w, 1 - x, y, s), X + s)
            receive(w, slot(w, 1 - x, 1 - y, 3 - near), CZ + 3 - near)
            send(w, WI.at[w, c, 1 - x], PP + 1, pp)

    def group_partner(w, rel):
        receive(w, WI.at[w, 1 - c, x if rel == 0 else 1 - x], PP + rel)

    def column(i):
        s = item_at[i]
        if i >= 2:
            receive(2, slot(2, x, 1 - y, s), Y + s)
            receive(2, slot(2, 1 - x, y, s), X + s)
        if i == 3:
            receive(2, slot(2, 1 - x, 1 - y, s), CZ + s)
        send(2, WO.at[c, s], PP + s, pp)

    def halo_copy(src, dst, sem, dev):
        return pltpu.make_async_remote_copy(
            src_ref=src,
            dst_ref=dst,
            send_sem=hs.at[sem],
            recv_sem=hr.at[sem],
            device_id=dev,
            device_id_type=MESH,
        )

    to_next = halo_copy(FR.at[pl.ds(rows - HALO, HALO), :], HB.at[0], 0, pn)
    to_before = halo_copy(FR.at[pl.ds(0, HALO), :], HB.at[1], 1, pb)

    def halo_start():
        @pl.when(has_next)
        def _():
            to_next.start()

        @pl.when(has_before)
        def _():
            to_before.start()

    def norm_rows(block):
        values = block.astype(jnp.float32)
        average = jnp.mean(values, axis=1, keepdims=True)
        centered = values - average
        spread_ = jnp.mean(centered * centered, axis=1, keepdims=True)
        return (centered * lax.rsqrt(spread_ + epsilon) * gain1[...]).astype(jnp.bfloat16)

    tall_rows = BLK
    pack = 2 * 8

    def tile(ref, first, ch):
        return ref[pl.ds(first, pack), ch * LANES : (ch + 1) * LANES].astype(jnp.float32)

    def row_sum(parts):
        total_ = parts[0]
        for part in parts[1:]:
            total_ = total_ + part
        return jnp.sum(total_, axis=1, keepdims=True)

    def norm(step):
        def bands(i):
            return [
                pl.multiple_of(i * tall_rows + r * pack, pack) for r in range(tall_rows // pack)
            ]

        def average_step(i, carry):
            for first in bands(i):
                average = row_sum([tile(FR, first, ch) for ch in range(chunks)]) / float(width)
                S1[pl.ds(first, pack), :] = jnp.broadcast_to(average, (pack, LANES))
            return carry

        def spread_step(i, carry):
            for first in bands(i):
                average = S1[pl.ds(first, pack), :]
                parts = [tile(FR, first, ch) - average for ch in range(chunks)]
                spread = row_sum([p * p for p in parts]) / float(width)
                scale = lax.rsqrt(spread + epsilon)
                S2[pl.ds(first, pack), :] = jnp.broadcast_to(scale, (pack, LANES))
            return carry

        def scale_step(i, carry):
            for first in bands(i):
                average = S1[pl.ds(first, pack), :]
                scale = S2[pl.ds(first, pack), :]
                for ch in range(chunks):
                    cols = slice(ch * LANES, (ch + 1) * LANES)
                    NM[pl.ds(first, pack), cols] = (
                        (tile(FR, first, ch) - average) * scale * gain1[:, cols]
                    ).astype(jnp.bfloat16)
            return carry

        count = rows // tall_rows // 2
        for stage in (average_step, spread_step, scale_step):
            lax.fori_loop(count * step, count * (step + 1), stage, 0)

    def halo():
        @pl.when(has_before)
        def _():
            to_next.wait_recv()

        @pl.when(has_next)
        def _():
            to_before.wait_recv()

        NH[0:HALO, :] = norm_rows(HB[0])
        NH[HALO:, :] = norm_rows(HB[1])

    first_block = index * nblk
    last_block = total * nblk - 1

    def block_info(b):
        u = utts[b]
        return u, lens[u] - offs[b] * BLK

    info = [
        block_info(jnp.clip(first_block + i, 0, last_block)) for i in range(-1, nblk + 1)
    ]
    joined = []
    for i in range(nblk + 1):
        same = info[i][0] == info[i + 1][0]
        if i == 0:
            same = same & (first_block > 0)
        if i == nblk:
            same = same & (first_block + nblk <= last_block)
        joined.append(same.astype(jnp.float32))
    alive_rows = [info[i + 1][1] for i in range(nblk)]
    for i in range(nblk):
        limits[i] = alive_rows[i]
    edge_limits[0] = info[0][1] - (BLK - HALO)
    edge_limits[1] = info[nblk + 1][1]
    edge_joined[0] = joined[0]
    edge_joined[1] = joined[nblk]

    def tall(count, start):
        return start + lax.broadcasted_iota(jnp.int32, (count, LANES), 0)

    stride = BLK + 2 * HALO

    def chunk_of(h, rel_c, rel_x):
        cc = c if rel_c == 0 else 1 - c
        xx = x if rel_x == 0 else 1 - x
        return cc, xx, (xx * 2 + cc) * 2 + h

    started = []
    pending = []
    deep = 4
    part_rows = 16 * deep
    parts = BLK // part_rows

    def convolve_step(j, ch, buf, fresh, tap):
        i, q = j // (2 * parts), j % (2 * parts)
        base = pl.multiple_of(i * stride + q * (8 * deep), 8)
        sums = [None] * deep
        for o in range(8 * (deep - 1) + KER):
            value = buf[pl.ds(base + (1 + o), 8), :]
            for t in range(deep):
                k = o - 8 * t
                if 0 <= k < KER:
                    term = value * tap[k]
                    sums[t] = term if sums[t] is None else sums[t] + term
        first = pl.multiple_of(j * (8 * deep), 8 * deep)
        for t in range(deep):
            band = pl.ds(pl.multiple_of(first + 8 * t, 8), 8)
            MX[ch, band, :] = sums[t]
            if fresh:
                S1[band, :] = sums[t]
                S2[band, :] = sums[t] * sums[t]
            else:
                S1[band, :] += sums[t]
                S2[band, :] += sums[t] * sums[t]

    def work(project_id):
        earlier = pending.pop() if pending else None
        if earlier is None and project_id is None:
            return
        if earlier is not None:
            old_ch, old_buf, fresh = earlier
            tap = [jnp.broadcast_to(TP[old_ch, k : k + 1, :], (8, LANES)) for k in range(KER)]
        if project_id is not None:
            h = project_id[0]
            cc, xx, ch = chunk_of(*project_id)
            buf = (GB0, GB1)[len(started) % 2]
            pending.append((ch, buf, not started))
            started.append(ch)

        def gated(p):
            half = 0.5 * p[:, :LANES]
            return half + half * jnp.tanh(0.5 * p[:, LANES:])

        def rounded(units):
            return units.astype(jnp.bfloat16).astype(jnp.float32)

        def at_once(between):
            lhs = jnp.concatenate([NM[...], NH[...]], axis=0)
            p = jnp.dot(lhs, WI[h, cc, xx], preferred_element_type=jnp.float32)
            between()
            units = gated(p)
            for i in range(nblk):
                main = jnp.where(tall(BLK, 0) < alive_rows[i], units[i * BLK : (i + 1) * BLK], 0.0)
                buf[i * stride + HALO : i * stride + HALO + BLK, :] = rounded(main)
            for q in range(2):
                strip = units[rows + q * HALO : rows + (q + 1) * HALO]
                strip = rounded(jnp.where(tall(HALO, 0) < edge_limits[q], strip, 0.0))
                place = q * (nblk * stride - HALO)
                buf[place : place + HALO, :] = strip * edge_joined[q]

        def convolve(steps):
            for j in steps:
                convolve_step(j, old_ch, old_buf, fresh, tap)

        count = 2 * nblk * parts
        if earlier is None:
            at_once(lambda: None)
        elif project_id is None:

            def step(j, carry):
                convolve((2 * j, 2 * j + 1))
                return carry

            lax.fori_loop(0, count // 2, step, 0)
        else:
            at_once(lambda: convolve(range(count)))
        if project_id is not None:
            for i in range(1, nblk):
                base = i * stride
                buf[base : base + HALO, :] = (
                    buf[base - 2 * HALO : base - HALO, :] * joined[i]
                )
                buf[base - HALO : base, :] = (
                    buf[base + HALO : base + 2 * HALO, :] * joined[i]
                )

    wide = 2 * LANES

    def finish_all():
        half = WO.shape[3] * WO.shape[4]
        for s in item_at:
            receive(2, WO.at[1 - c, s], PP + s)
        if not COMPUTE:
            return
        for b in range(nblk):
            stats = []
            for r in range(tall_rows // pack):
                band = slice(b * BLK + r * pack, b * BLK + (r + 1) * pack)
                average = jnp.sum(S1[band, :], axis=1, keepdims=True) / float(width)
                square = jnp.sum(S2[band, :], axis=1, keepdims=True) / float(width)
                scale = lax.rsqrt(square - average * average + epsilon)
                stats.append((band, average, scale))
            for ch in range(chunks):
                cols = slice(ch * LANES, (ch + 1) * LANES)
                g, h = ch // 2, ch % 2
                place = ((g % 2) * 2 + g // 2) * 2 + h
                half_gain = 0.5 * gain2[:, cols]
                half_bias = 0.5 * bias2[:, cols]
                for band, average, scale in stats:
                    v = (MX[ch, band, :] - average) * scale * half_gain + half_bias
                    ACT[band, place * LANES : (place + 1) * LANES] = (
                        v + v * jnp.tanh(v)
                    ).astype(jnp.bfloat16)
            band = slice(b * BLK, (b + 1) * BLK)
            lived = lax.broadcasted_iota(jnp.int32, (BLK, wide), 0) < alive_rows[b]
            for s in item_at:

                def side(sy):
                    return jnp.concatenate(
                        [WO[cc, s, sy].reshape(half, LANES) for cc in range(2)], axis=0
                    )

                weights = jnp.concatenate([side(0), side(1)], axis=1)
                o = jnp.dot(ACT[band, :], weights, preferred_element_type=jnp.float32)
                cols = pl.ds(pl.multiple_of(s * wide, wide), wide)
                out[band, cols] = (
                    FR[band, cols].astype(jnp.float32) + jnp.where(lived, o, 0.0)
                ).astype(jnp.bfloat16)

    for token in ORDER:
        arg = [int(d) for d in token if d.isdigit()]
        name = token.rstrip("0123456789")
        if name == "Q":
            own_square(*arg)
        elif name == "R":
            own_line(*arg)
            if arg[0] == 0:
                load.wait()
                halo_start()
                for ch in range(chunks):
                    TP[ch, 0:KER, :] = taps[:, ch * LANES : (ch + 1) * LANES].astype(
                        jnp.float32
                    )
        elif name == "B":
            line(*arg)
        elif name == "XY":
            corner_sends(*arg)
        elif name == "C":
            corner(*arg)
        elif name == "D":
            corner_relay(*arg)
        elif name == "G":
            group(arg[1], arg[0])
        elif name == "P":
            group_partner(arg[1], arg[0])
        elif name == "S":
            column(*arg)
        elif name == "fin":
            finish_all()
        elif name == "halo":
            halo()
        elif not COMPUTE:
            pass
        elif name == "K":
            work(arg)
        elif name == "L":
            work(None)
        elif name == "N":
            norm(*arg)

    if not COMPUTE:
        out[...] = FR[...]

    @pl.when(has_next)
    def _():
        to_next.wait_send()

    @pl.when(has_before)
    def _():
        to_before.wait_send()

    for made in sent:
        made.wait_send()

    @pl.when(end == 0)
    def _():
        for made in middle_sent:
            made.wait_send()


def fused_device(
    frames, ln1_gain, w_in, w_dw, ln2_gain, ln2_bias, w_out, block_utt, block_off, lengths
):
    rows, width = frames.shape
    nz = lax.axis_size("seq") // 2
    krows, _, cols = w_in.shape
    orows, ocols = w_out.shape
    groups = cols // LANES
    wi = w_in.reshape(krows, 2, groups, LANES).transpose(0, 2, 1, 3).reshape(krows, 2 * cols)
    vmem = pl.BlockSpec(memory_space=pltpu.VMEM)
    smem = pl.BlockSpec(memory_space=pltpu.SMEM)
    anywhere = pl.BlockSpec(memory_space=pl.ANY)
    nblk = rows // BLK
    return pl.pallas_call(
        fused_kernel,
        out_shape=jax.ShapeDtypeStruct((rows, width), jnp.bfloat16),
        in_specs=[anywhere] + [vmem] * 6 + [smem] * 3,
        out_specs=vmem,
        scratch_shapes=[
            pltpu.VMEM((2, 2, 2, width, 2 * LANES), jnp.bfloat16),
            pltpu.VMEM((2, nz, 2, 2, orows, ocols), jnp.bfloat16),
            pltpu.VMEM((rows, width), jnp.bfloat16),
            pltpu.VMEM((2, HALO, width), jnp.bfloat16),
            pltpu.VMEM((rows, width), jnp.bfloat16),
            pltpu.VMEM((2 * HALO, width), jnp.bfloat16),
            pltpu.VMEM((nblk * (BLK + 2 * HALO), LANES), jnp.float32),
            pltpu.VMEM((nblk * (BLK + 2 * HALO), LANES), jnp.float32),
            pltpu.VMEM((width // LANES, rows, LANES), jnp.float32),
            pltpu.VMEM((width // LANES, 32, LANES), jnp.float32),
            pltpu.VMEM((rows, width), jnp.bfloat16),
            pltpu.VMEM((rows, LANES), jnp.float32),
            pltpu.VMEM((rows, LANES), jnp.float32),
            pltpu.SMEM((nblk,), jnp.int32),
            pltpu.SMEM((2,), jnp.int32),
            pltpu.SMEM((2,), jnp.float32),
            pltpu.SemaphoreType.DMA((3, KINDS)),
            pltpu.SemaphoreType.DMA((3, KINDS)),
            pltpu.SemaphoreType.DMA((2,)),
            pltpu.SemaphoreType.DMA((2,)),
            pltpu.SemaphoreType.DMA((1,)),
        ],
        compiler_params=pltpu.CompilerParams(
            collective_id=0, has_side_effects=True, vmem_limit_bytes=52 << 20
        ),
    )(
        frames,
        wi,
        w_out,
        ln1_gain[None],
        w_dw,
        ln2_gain[None],
        ln2_bias[None],
        block_utt,
        block_off,
        lengths,
    )


def solution(mesh):
    seq, grp = mesh.shape["seq"], mesh.shape["grp"]
    fits = grp == 4 and seq == 2 * PLANES and D == grp * 2 * LANES

    return jax.shard_map(
        fused_device if fits else per_device,
        mesh=mesh,
        in_specs=(
            P(("seq", "grp"), None),
            P(),
            P("seq", None, "grp"),
            P(),
            P(),
            P(),
            P("grp", "seq"),
            P(),
            P(),
            P(),
        ),
        out_specs=P(("seq", "grp"), None),
        check_vma=False,
    )
```
